128 devices in a mesh: role: 2 (over core), tok: 64 (over y, x, z).
Axes of the slice: x: 4, y: 4, z: 4, core: 2. Of those that a mesh axis runs over, the one named last changes fastest.
Arguments:
- hidden: bfloat16 [16384, 2048], P('tok'), may hold values from -6 to 6
- doc_blocks: int32 [10], replicated, may hold values from 1 to 16, 128 in all
- norm_gain: float32 [2048], replicated, may hold values from 0.5 to 2
- w_query: bfloat16 [2048, 4096], P(None, 'role'), may hold values from -0.125 to 0.125
- w_key: bfloat16 [2048, 512], P(None, 'role'), may hold values from -0.125 to 0.125
- w_value: bfloat16 [2048, 512], P(None, 'role'), may hold values from -0.125 to 0.125
- q_gain: float32 [128], replicated, may hold values from 0.5 to 6
- k_gain: float32 [128], replicated, may hold values from 0.5 to 6
- w_out: bfloat16 [4096, 2048], P('role'), may hold values from -0.09375 to 0.09375
Outputs:
- attn_out: bfloat16 [16384, 2048], P('tok', 'role')
The draws below stay inside these ranges and needn't reach their ends.
All inputs are finite; a program needn't handle non-finite values.
Results may differ from the reference program's by a relative error of at most 0.006.
The reference program's roundings to bfloat16 on the way count: a program that leaves them out, or rounds other values in their place, can miss the bound.
Values may be sent and summed in bfloat16 or wider, within the bound.
No kernel may reach another device: no remote copies, remote signals or barrier semaphores. Data moves between devices by JAX's collectives and lax.ppermute only.
A program may use at most 192 MiB of HBM per device.

```python
import math
import jax
import jax.numpy as jnp
import numpy as np
from jax import lax

D = 2048
HQ = 32
HK = 4
HD = 128
BLK = 128
MOST = 16
NBLK = 128
TOKENS = 16384
NDOCS = 10


def draw_gain_common(key, salt):
    local_key = jax.random.fold_in(key, salt)
    return jnp.exp(jax.random.uniform(local_key, (HD,), jnp.float32, jnp.log(0.5), jnp.log(2.0)))


def draw_q_gain(key, part):
    return draw_gain_common(key, 11)


def draw_k_gain(key, part):
    return draw_gain_common(key, 23)


def shard_levels(rng, extent, cuts, low, top_value):
    loudness = 1.0
    for axis_at, parts in cuts:
        heights = jax.random.uniform(jax.random.fold_in(jax.random.fold_in(rng, 6), axis_at), (parts,), jnp.float32, low / len(cuts), top_value / len(cuts))
        loudness = loudness * jnp.repeat(jnp.exp(heights), extent[axis_at] // parts).reshape((-1,) + (1,) * (len(extent) - 1 - axis_at))
    return loudness


def length_profile(count, total, most, slope):
    loads = [(1 << 20) // math.isqrt(rank ** slope) + 1 for rank in range(2, count + 1)]
    spare, holding = total - most - (count - 1), [1] * (count - 1)
    while spare > 0:
        free = [i for i in range(count - 1) if holding[i] < most]
        pool, left = sum([loads[i] for i in free]), spare
        for i in free:
            addition = min(most - holding[i], max(1, left * loads[i] // pool), spare)
            holding[i] = holding[i] + addition
            spare = spare - addition
    return np.array([most] + holding)


def ragged(own_key, number_of, total, reach, lean):
    if number_of == 2:
        one = jax.random.randint(own_key, (), max(1, total - reach), min(reach, total - 1) + 1)
        return jnp.stack([one, total - one])
    sizes = jnp.asarray(length_profile(number_of, total, reach, lean), jnp.int32)
    couples = (number_of - 1) // 2
    source_of, sink = sizes[1:1 + 2 * couples:2], sizes[2:2 + 2 * couples:2]
    slack = jnp.minimum(source_of - 1, reach - sink)
    passed = jax.random.randint(jax.random.fold_in(own_key, 1), (couples,), 0, 1 << 20) % (slack + 1)
    sizes = sizes.at[1:1 + 2 * couples:2].set(source_of - passed).at[2:2 + 2 * couples:2].set(sink + passed)
    return sizes[jax.random.permutation(jax.random.fold_in(own_key, 2), number_of)]


def gaussian(key, shape, scale, limit, cuts=(), kind=jnp.bfloat16):
    gain = shard_levels(key, shape, cuts, -0.22, 0.18) if cuts else 1.0
    result = jax.random.normal(key, shape, jnp.float32) * scale * gain
    return jnp.minimum(jnp.maximum(result, -limit), limit).astype(kind)


def setup_inputs(seed: int = 0) -> dict:
    seeds = jax.random.split(jax.random.key(seed), 10)
    return {
        "hidden": gaussian(seeds[0], (TOKENS, D), 1.0, 6.0, ((0, 64),)),
        "doc_blocks": ragged(seeds[1], NDOCS, NBLK, MOST, 1).astype(jnp.int32),
        "norm_gain": jnp.clip(jnp.exp(jax.random.uniform(seeds[2], (D,), jnp.float32, math.log(0.5), math.log(2.0))), 0.5, 2.0),
        "w_query": gaussian(seeds[3], (D, HQ * HD), D ** -0.5, 0.125, ((1, 2),)),
        "w_key": gaussian(seeds[4], (D, HK * HD), D ** -0.5, 0.125, ((1, 2),)),
        "w_value": gaussian(seeds[5], (D, HK * HD), D ** -0.5, 0.125, ((1, 2),)),
        "q_gain": draw_q_gain(jax.random.fold_in(seeds[9], 71), 0),
        "k_gain": draw_k_gain(jax.random.fold_in(seeds[9], 71), 0),
        "w_out": gaussian(seeds[8], (HQ * HD, D), (HQ * HD) ** -0.5, 0.09375, ((0, 2),)),
    }


EPSILON = 1e-06
THETA = 1000000.0

def rms_scale(values, gain_row):
    mean_sq = lax.optimization_barrier(jnp.mean(values * values, axis=-1, keepdims=True))
    return values * lax.rsqrt(mean_sq + EPSILON) * gain_row

def rotate(values, positions):
    width = values.shape[-1]
    half_width = width // 2
    frequency = THETA ** (-(jnp.arange(half_width, dtype=jnp.float32) * 2.0) / width)
    angle_table = positions.astype(jnp.float32)[:, None] * frequency[None, :]
    cosine = jnp.concatenate([jnp.cos(angle_table), jnp.cos(angle_table)], axis=-1)[:, None, :]
    sine_table = jnp.concatenate([jnp.sin(angle_table), jnp.sin(angle_table)], axis=-1)[:, None, :]
    first_half = values[..., :half_width]
    second_half = values[..., half_width:]
    turned = jnp.concatenate([-second_half, first_half], axis=-1)
    return values * cosine + turned * sine_table

def block_layout(doc_blocks, total_blocks):
    doc_ends = jnp.cumsum(doc_blocks).astype(jnp.int32)
    doc_starts = (doc_ends - doc_blocks).astype(jnp.int32)
    block_ids = jnp.arange(total_blocks, dtype=jnp.int32)
    doc_of = lax.optimization_barrier(jnp.sum((block_ids[:, None] >= doc_ends[None, :]).astype(jnp.int32), axis=1)).astype(jnp.int32)
    doc_numbers = jnp.arange(doc_blocks.shape[0], dtype=jnp.int32)
    start_of = lax.optimization_barrier(jnp.sum(jnp.where(doc_of[:, None] == doc_numbers[None, :], doc_starts[None, :], 0), axis=1)).astype(jnp.int32)
    return (doc_of, start_of)

def reference(hidden, doc_blocks, norm_gain, w_query, w_key, w_value, q_gain, k_gain, w_out):
    tokens = hidden.shape[0]
    total_blocks = tokens // BLK
    doc_of, start_of = block_layout(doc_blocks, total_blocks)
    token_ids = jnp.arange(tokens, dtype=jnp.int32)
    token_doc = jnp.repeat(doc_of, BLK).astype(jnp.int32)
    positions = (token_ids - jnp.repeat(start_of, BLK) * BLK).astype(jnp.int32)
    normed = rms_scale(hidden.astype(jnp.float32), norm_gain).astype(jnp.bfloat16)
    queries = jnp.dot(normed, w_query, preferred_element_type=jnp.float32).reshape(tokens, HQ, HD)
    queries = rotate(rms_scale(queries, q_gain), positions).astype(jnp.bfloat16)
    keys_all = jnp.dot(normed, w_key, preferred_element_type=jnp.float32).reshape(tokens, HK, HD)
    keys_all = rotate(rms_scale(keys_all, k_gain), positions).astype(jnp.bfloat16)
    values_all = jnp.dot(normed, w_value, preferred_element_type=jnp.float32).astype(jnp.bfloat16).reshape(tokens, HK, HD)
    span_keys = MOST * BLK
    lead_rows = (MOST - 1) * BLK
    key_pad = jnp.concatenate([jnp.zeros((lead_rows, HK, HD), jnp.bfloat16), keys_all], axis=0)
    value_pad = jnp.concatenate([jnp.zeros((lead_rows, HK, HD), jnp.bfloat16), values_all], axis=0)
    doc_pad = jnp.concatenate([jnp.full((lead_rows,), -1, jnp.int32), token_doc], axis=0)
    group_size = HQ // HK
    scale = HD ** (-0.5)

    def one_block(block_id):
        first_row = (block_id * BLK).astype(jnp.int32)
        q_rows = lax.dynamic_slice_in_dim(queries, first_row, BLK, 0)
        k_rows = lax.dynamic_slice_in_dim(key_pad, first_row, span_keys, 0)
        v_rows = lax.dynamic_slice_in_dim(value_pad, first_row, span_keys, 0)
        k_doc = lax.dynamic_slice_in_dim(doc_pad, first_row, span_keys, 0)
        q_doc = lax.dynamic_slice_in_dim(token_doc, first_row, BLK, 0)
        q_index = first_row + jnp.arange(BLK, dtype=jnp.int32)
        k_index = first_row - lead_rows + jnp.arange(span_keys, dtype=jnp.int32)
        allowed = (k_doc[None, :] == q_doc[:, None]) & (k_index[None, :] <= q_index[:, None])
        q_float = q_rows.astype(jnp.float32).reshape(BLK, HK, group_size, HD)
        scores = jnp.einsum('tkgd,skd->kgts', q_float, k_rows.astype(jnp.float32)) * scale
        masked = jnp.where(allowed[None, None], scores, -1e+30)
        row_top = lax.optimization_barrier(jnp.max(masked, axis=-1, keepdims=True))
        weights = jnp.where(allowed[None, None], jnp.exp(masked - row_top), 0.0)
        weights = (weights / lax.optimization_barrier(jnp.sum(weights, axis=-1, keepdims=True))).astype(jnp.bfloat16)
        mixed_rows = jnp.einsum('kgts,skd->tkgd', weights.astype(jnp.float32), v_rows.astype(jnp.float32))
        return mixed_rows.reshape(BLK, HQ * HD).astype(jnp.bfloat16)
    attended = lax.map(one_block, jnp.arange(total_blocks, dtype=jnp.int32)).reshape(tokens, HQ * HD)
    return jnp.dot(attended, w_out, preferred_element_type=jnp.float32).astype(jnp.bfloat16)
```

```python
import functools

import numpy as np
import jax
import jax.numpy as jnp
from jax import lax
from jax.experimental import pallas as pl
from jax.experimental.pallas import tpu as pltpu
from jax.sharding import PartitionSpec as P

HD = 128
BLK = 128
MOST = 16
NDOCS = 10
EPSILON = 1e-06
THETA = 1000000.0
TOK = 256
CHUNKS = 9
BF = jnp.bfloat16
F32 = jnp.float32
SCALE2 = float(HD ** (-0.5) * np.log2(np.e))


def doc_start(docs, block):
    end = jnp.int32(0)
    start = jnp.int32(0)
    for j in range(NDOCS):
        end = end + docs[j]
        start = jnp.where(end <= block, end, start)
    return start


def head_norm_rope(x, gain, cos, sin):
    ms = jnp.mean(x * x, axis=-1, keepdims=True)
    x = x * lax.rsqrt(ms + EPSILON) * gain
    return (x * cos + pltpu.roll(x, HD // 2, 1) * sin).astype(BF)


def kv_kernel(docs, hid, ngain, wk, wv, kgain, freq, normed_o, kv_o, cos_o, sin_o):
    first = lax.axis_index("tok") * 2
    s0 = doc_start(docs, first) * BLK
    s1 = doc_start(docs, first + 1) * BLK
    row = lax.broadcasted_iota(jnp.int32, (TOK, HD), 0)
    pos = first * BLK + row - jnp.where(row < BLK, s0, s1)
    ang = pos.astype(F32) * freq[...]
    cos = jnp.cos(ang)
    lane = lax.broadcasted_iota(jnp.int32, (TOK, HD), 1)
    sin = jnp.sin(ang)
    sin = jnp.where(lane < HD // 2, -sin, sin)
    cos_o[...] = cos
    sin_o[...] = sin
    x = hid[...].astype(F32)
    ms = jnp.mean(x * x, axis=-1, keepdims=True)
    normed = (x * lax.rsqrt(ms + EPSILON) * ngain[...]).astype(BF)
    normed_o[...] = normed
    k = jnp.dot(normed, wk[...], preferred_element_type=F32)
    for h in range(2):
        kv_o[0, :, h * HD:(h + 1) * HD] = head_norm_rope(
            k[:, h * HD:(h + 1) * HD], kgain[...], cos, sin)
    kv_o[1] = jnp.dot(normed, wv[...], preferred_element_type=F32).astype(BF)


def q_kernel(normed, wq, qgain, cos, sin, q_o):
    q = jnp.dot(normed[...], wq[...], preferred_element_type=F32)
    for h in range(q.shape[1] // HD):
        q_o[h] = head_norm_rope(q[:, h * HD:(h + 1) * HD], qgain[...], cos[...], sin[...])


def attend_kernel(docs, q, *rest):
    pieces = rest[:CHUNKS]
    wout = rest[CHUNKS]
    send_o, keep_o = rest[CHUNKS + 1:CHUNKS + 3]
    win, wbuf, m_s, acc_s, att, sems, wsem = rest[CHUNKS + 3:]
    me = lax.axis_index("tok")
    role = lax.axis_index("role")
    wcopy = pltpu.make_async_copy(wout, wbuf, wsem)
    copies = [pltpu.make_async_copy(pieces[c], win.at[c], sems.at[c]) for c in range(CHUNKS)]
    for c in range(CHUNKS):
        copies[c].start()
    wcopy.start()
    for c in range(CHUNKS):
        copies[c].wait()

    def tile(g, i, chunk, lo, size, mask, first):
        qv = q[g * 8:(g + 1) * 8, i * BLK:(i + 1) * BLK, :].reshape(8 * BLK, HD)
        k = win[chunk, 0, lo:lo + size, g * HD:(g + 1) * HD]
        v = win[chunk, 1, lo:lo + size, g * HD:(g + 1) * HD]
        v1 = jnp.concatenate([v, jnp.ones((size, HD), BF)], axis=1)
        s = lax.dot_general(qv, k, (((1,), (1,)), ((), ())), preferred_element_type=F32)
        if mask is not None:
            s = jnp.where(mask, s, -1e30)
        top = jnp.max(s, axis=-1, keepdims=True)
        if first:
            m_new = top
        else:
            m_old = m_s[:, :1]
            m_new = jnp.maximum(m_old, top)
        p = jnp.exp2((s - m_new) * SCALE2).astype(BF)
        pv = jnp.dot(p, v1, preferred_element_type=F32)
        if first:
            acc_s[...] = pv
        else:
            acc_s[...] = acc_s[...] * jnp.exp2((m_old - m_new) * SCALE2) + pv
        m_s[...] = jnp.broadcast_to(m_new, (8 * BLK, HD))

    for i in range(2):
        block = me * 2 + i
        depth = block - doc_start(docs, block)
        start = 2 * (CHUNKS - 1) + i - depth
        for g in range(2):
            size = BLK * (i + 1)
            row = lax.broadcasted_iota(jnp.int32, (8, BLK, size), 1).reshape(8 * BLK, size)
            col = lax.broadcasted_iota(jnp.int32, (8, BLK, size), 2).reshape(8 * BLK, size)
            mask = col <= row + i * BLK
            if i == 1:
                mask = mask & (col >= jnp.where(depth == 0, BLK, 0))
            tile(g, i, CHUNKS - 1, 0, size, mask, True)

            @pl.when((start % 2 == 1) & (start < 2 * (CHUNKS - 1)))
            def _():
                tile(g, i, start // 2, BLK, BLK, None, False)

            @pl.loop((start + 1) // 2, CHUNKS - 1)
            def _(chunk):
                tile(g, i, chunk, 0, 2 * BLK, None, False)

            o = (acc_s[:, :HD] / acc_s[:, HD:]).astype(BF)
            for h in range(8):
                att[i * BLK:(i + 1) * BLK, (g * 8 + h) * HD:(g * 8 + h + 1) * HD] = o[h * BLK:(h + 1) * BLK]
    wcopy.wait()
    half = wout.shape[1] // 2
    a = att[...]
    theirs = pl.multiple_of((1 - role) * half, half)
    mine = pl.multiple_of(role * half, half)
    send_o[...] = jnp.dot(a, wbuf[:, pl.ds(theirs, half)], preferred_element_type=F32).astype(BF)
    keep_o[...] = jnp.dot(a, wbuf[:, pl.ds(mine, half)], preferred_element_type=F32)


SMEM = pl.BlockSpec(memory_space=pltpu.MemorySpace.SMEM)
ANY = pl.BlockSpec(memory_space=pl.ANY)
VM = pl.BlockSpec(memory_space=pltpu.MemorySpace.VMEM)


def shifted(value, by):
    peers = lax.axis_size("tok")
    return lax.ppermute(value, "tok", [(i, (i + by) % peers) for i in range(peers)])


def on_device(hidden, doc_blocks, norm_gain, w_query, w_key, w_value, q_gain, k_gain, w_out):
    d = hidden.shape[1]
    hq = w_query.shape[1] // HD
    freq = THETA ** (-(np.arange(HD // 2, dtype=np.float32) * np.float32(2.0)) / np.float32(HD))
    freq = jnp.asarray(np.concatenate([freq, freq])[None].astype(np.float32))
    normed, kv, cos, sin = pl.pallas_call(
        kv_kernel,
        out_shape=(
            jax.ShapeDtypeStruct((TOK, d), BF),
            jax.ShapeDtypeStruct((2, TOK, 2 * HD), BF),
            jax.ShapeDtypeStruct((TOK, HD), F32),
            jax.ShapeDtypeStruct((TOK, HD), F32),
        ),
        in_specs=[SMEM] + [VM] * 6,
        out_specs=[VM] * 4,
        cost_estimate=pl.CostEstimate(flops=540_000_000, transcendentals=0, bytes_accessed=4_000_000),
        name="kv_kernel",
    )(doc_blocks, hidden, norm_gain[None], w_key, w_value, k_gain[None], freq)

    pieces = [shifted(kv, CHUNKS - 1 - w) for w in range(CHUNKS - 1)] + [kv]

    cols = 512
    queries = pl.pallas_call(
        q_kernel,
        grid=(w_query.shape[1] // cols,),
        out_shape=jax.ShapeDtypeStruct((hq, TOK, HD), BF),
        in_specs=[
            pl.BlockSpec((TOK, d), lambda j: (0, 0)),
            pl.BlockSpec((d, cols), lambda j: (0, j)),
            pl.BlockSpec((1, HD), lambda j: (0, 0)),
            pl.BlockSpec((TOK, HD), lambda j: (0, 0)),
            pl.BlockSpec((TOK, HD), lambda j: (0, 0)),
        ],
        out_specs=pl.BlockSpec((cols // HD, TOK, HD), lambda j: (j, 0, 0)),
        cost_estimate=pl.CostEstimate(flops=2_147_000_000, transcendentals=0, bytes_accessed=10_000_000),
        name="q_kernel",
    )(normed, w_query, q_gain[None], cos, sin)

    half = w_out.shape[1] // 2
    send, keep = pl.pallas_call(
        attend_kernel,
        out_shape=(
            jax.ShapeDtypeStruct((TOK, half), BF),
            jax.ShapeDtypeStruct((TOK, half), F32),
        ),
        in_specs=[SMEM, VM] + [ANY] * (CHUNKS + 1),
        out_specs=[VM, VM],
        scratch_shapes=[
            pltpu.VMEM((CHUNKS, 2, TOK, 2 * HD), BF),
            pltpu.VMEM(w_out.shape, BF),
            pltpu.VMEM((8 * BLK, HD), F32),
            pltpu.VMEM((8 * BLK, 2 * HD), F32),
            pltpu.VMEM((TOK, hq * HD), BF),
            pltpu.SemaphoreType.DMA((CHUNKS,)),
            pltpu.SemaphoreType.DMA,
        ],
        cost_estimate=pl.CostEstimate(flops=12_000_000_000, transcendentals=0, bytes_accessed=14_000_000),
        name="attend_kernel",
    )(doc_blocks, queries, *pieces, w_out)
    other = lax.ppermute(send, "role", [(0, 1), (1, 0)])
    return (keep + other.astype(F32)).astype(BF)


def solution(mesh):
    return jax.shard_map(
        on_device,
        mesh=mesh,
        in_specs=(
            P("tok", None), P(), P(), P(None, "role"), P(None, "role"), P(None, "role"),
            P(), P(), P("role", None),
        ),
        out_specs=P("tok", "role"),
        check_vma=False,
    )
```

```python
import functools

import numpy as np
import jax
import jax.numpy as jnp
from jax import lax
from jax.experimental import pallas as pl
from jax.experimental.pallas import tpu as pltpu
from jax.sharding import PartitionSpec as P

HD = 128
BLK = 128
MOST = 16
NDOCS = 10
EPSILON = 1e-06
THETA = 1000000.0
TOK = 256
RING = 4
EXTRA = 16
AHEAD = 2
BF = jnp.bfloat16
F32 = jnp.float32
SCALE2 = float(HD ** (-0.5) * np.log2(np.e))


def doc_start(docs, block):
    end = jnp.int32(0)
    start = jnp.int32(0)
    for j in range(NDOCS):
        end = end + docs[j]
        start = jnp.where(end <= block, end, start)
    return start


def head_norm_rope(x, gain, cos, sin):
    ms = jnp.mean(x * x, axis=-1, keepdims=True)
    x = x * lax.rsqrt(ms + EPSILON) * gain
    return (x * cos + pltpu.roll(x, HD // 2, 1) * sin).astype(BF)


def head_norm_rope_t(x, gain, cos, sin):
    ms = jnp.mean(x * x, axis=0, keepdims=True)
    x = x * lax.rsqrt(ms + EPSILON) * gain
    turned = jnp.concatenate([x[HD // 2:], x[:HD // 2]], axis=0)
    return (x * cos + turned * sin).astype(BF)


def kv_kernel(docs, hid, ngain, wk, wv, kgain, freq, normed_o, kv_o, cos_o, sin_o):
    first = lax.axis_index("tok") * 2
    s0 = doc_start(docs, first) * BLK
    s1 = doc_start(docs, first + 1) * BLK
    row = lax.broadcasted_iota(jnp.int32, (TOK, HD), 0)
    pos = first * BLK + row - jnp.where(row < BLK, s0, s1)
    ang = pos.astype(F32) * freq[...]
    cos = jnp.cos(ang)
    lane = lax.broadcasted_iota(jnp.int32, (TOK, HD), 1)
    sin = jnp.sin(ang)
    sin = jnp.where(lane < HD // 2, -sin, sin)
    cos_o[...] = cos.T
    sin_o[...] = sin.T
    x = hid[...].astype(F32)
    ms = jnp.mean(x * x, axis=-1, keepdims=True)
    normed = (x * lax.rsqrt(ms + EPSILON) * ngain[...]).astype(BF)
    normed_o[...] = normed
    k = jnp.dot(normed, wk[...], preferred_element_type=F32)
    for h in range(2):
        kv_o[0, :, h * HD:(h + 1) * HD] = head_norm_rope(
            k[:, h * HD:(h + 1) * HD], kgain[...], cos, sin)
    kv_o[1] = jnp.dot(normed, wv[...], preferred_element_type=F32).T.astype(BF)


def q_kernel(normed, wq, qgain, cos, sin, q_o):
    q = jnp.dot(normed[...], wq[...], preferred_element_type=F32)
    gain = jnp.broadcast_to(qgain[...], (TOK, HD)).T
    for h in range(q.shape[1] // HD):
        q_o[h] = head_norm_rope_t(q[:, h * HD:(h + 1) * HD].T, gain, cos[...], sin[...])


def attend_kernel(table, first_stage, last_stage, *refs):
    slots = len(table)
    refs = list(refs)
    docs, q = refs[:2]
    refs = refs[2:]
    pieces, refs = refs[:slots], refs[slots:]
    me = lax.axis_index("tok")
    role = lax.axis_index("role")
    if first_stage:
        own, refs = refs[0], refs[1:]
    else:
        m_in, acc_in, wout = refs[:3]
        refs = refs[3:]
    if last_stage:
        send_o, keep_o, win, hops, m_s, acc_s, att, wbuf, sems, wsem = refs
        wcopy = pltpu.make_async_copy(wout, wbuf, wsem)
    else:
        m_s, acc_s, win, hops, sems = refs
    sources = list(pieces) + ([own] if first_stage else [])
    copies = [pltpu.make_async_copy(p, win.at[n], sems.at[n]) for n, p in enumerate(sources)]
    for c in copies:
        c.start()
    if last_stage:
        wcopy.start()
    z = me % RING
    for n, row in enumerate(table):
        hop = jnp.int32(row[0])
        for zz in range(1, RING):
            hop = jnp.where(z == zz, jnp.int32(row[zz]), hop)
        hops[n] = hop
    if not first_stage:
        m_s[...] = m_in[...]
        acc_s[...] = acc_in[...]
    for c in copies:
        c.wait()
    step = 2 * BLK

    def tile(i, slot, lo, size, mask, first):
        units = [(g, j) for g in range(2) for j in range(4)]

        def scores(g, j):
            k = win[slot, 0, lo:lo + size, g * HD:(g + 1) * HD]
            qt = jnp.concatenate(
                [q[g * 8 + 2 * j + e, :, i * BLK:(i + 1) * BLK] for e in range(2)], axis=1)
            s = jnp.dot(k, qt, preferred_element_type=F32)
            return s if mask is None else jnp.where(mask, s, -1e30)

        ahead = [scores(*units[n]) for n in range(AHEAD)]
        for n, (g, j) in enumerate(units):
            s = ahead.pop(0)
            if n + AHEAD < len(units):
                ahead.append(scores(*units[n + AHEAD]))
            cols = slice(j * step, (j + 1) * step)
            v = win[slot, 1, g * HD:(g + 1) * HD, lo:lo + size]
            v1 = jnp.concatenate([v, jnp.ones((EXTRA, size), BF)], axis=0)
            top = jnp.max(s, axis=0, keepdims=True)
            if first:
                m_new = top
            else:
                m_old = m_s[i, g, :, cols]
                m_new = jnp.maximum(m_old, top)
            p = jnp.exp2((s - m_new) * SCALE2).astype(BF)
            pv = jnp.dot(v1, p, preferred_element_type=F32)
            if first:
                acc_s[i, g, :, cols] = pv
            else:
                acc_s[i, g, :, cols] = acc_s[i, g, :, cols] * jnp.exp2((m_old - m_new) * SCALE2) + pv
            m_s[i, g, :, cols] = m_new

    for i in range(2):
        block = me * 2 + i
        depth = block - doc_start(docs, block)
        if first_stage:
            size = BLK * (i + 1)
            key = lax.broadcasted_iota(jnp.int32, (size, step), 0)
            token = lax.broadcasted_iota(jnp.int32, (size, step), 1) % BLK
            mask = key <= token + i * BLK
            if i == 1:
                mask = mask & (key >= jnp.where(depth == 0, BLK, 0))
            tile(i, slots, 0, size, mask, True)

        @pl.loop(0, slots)
        def _(slot):
            hop = hops[slot]

            @pl.when((hop > 0) & (2 * hop + i <= depth))
            def _():
                tile(i, slot, 0, 2 * BLK, None, False)

            @pl.when((hop > 0) & (2 * hop + i == depth + 1))
            def _():
                tile(i, slot, BLK, BLK, None, False)

        if last_stage:
            for g in range(2):
                for h in range(8):
                    cols = slice(h * BLK, (h + 1) * BLK)
                    o = acc_s[i, g, :HD, cols] / acc_s[i, g, HD:HD + 1, cols]
                    att[i * BLK:(i + 1) * BLK, (g * 8 + h) * HD:(g * 8 + h + 1) * HD] = o.T.astype(BF)
    if last_stage:
        wcopy.wait()
        half = wout.shape[1] // 2
        a = att[...]
        theirs = pl.multiple_of((1 - role) * half, half)
        mine = pl.multiple_of(role * half, half)
        send_o[...] = jnp.dot(a, wbuf[:, pl.ds(theirs, half)], preferred_element_type=F32).astype(BF)
        keep_o[...] = jnp.dot(a, wbuf[:, pl.ds(mine, half)], preferred_element_type=F32)


SMEM = pl.BlockSpec(memory_space=pltpu.MemorySpace.SMEM)
ANY = pl.BlockSpec(memory_space=pl.ANY)
VM = pl.BlockSpec(memory_space=pltpu.MemorySpace.VMEM)


def moved(value, rows, turn, senders=(0, 1, 2, 3)):
    peers = lax.axis_size("tok")
    pairs = []
    for t in range(peers):
        z = t % RING
        if z in senders:
            pairs.append((t, (t - z + (z + turn) % RING + rows * RING) % peers))
    return lax.ppermute(value, "tok", pairs)


LEVEL1 = ((4, 4, 4, 4), (0, 1, 1, 1), (0, 0, 0, 3), (8, 8, 8, 8), (0, 0, 2, 2))
LEVEL2 = ((1, 5, 5, 5), (3, 3, 3, 7), (2, 2, 6, 6), (7, 7, 7, 0), (5, 0, 0, 0), (6, 6, 0, 0))


def on_device(hidden, doc_blocks, norm_gain, w_query, w_key, w_value, q_gain, k_gain, w_out):
    d = hidden.shape[1]
    hq = w_query.shape[1] // HD
    freq = THETA ** (-(np.arange(HD // 2, dtype=np.float32) * np.float32(2.0)) / np.float32(HD))
    freq = jnp.asarray(np.concatenate([freq, freq])[None].astype(np.float32))
    normed, kv, cos, sin = pl.pallas_call(
        kv_kernel,
        out_shape=(
            jax.ShapeDtypeStruct((TOK, d), BF),
            jax.ShapeDtypeStruct((2, TOK, 2 * HD), BF),
            jax.ShapeDtypeStruct((HD, TOK), F32),
            jax.ShapeDtypeStruct((HD, TOK), F32),
        ),
        in_specs=[SMEM] + [VM] * 6,
        out_specs=[VM] * 4,
        cost_estimate=pl.CostEstimate(flops=540_000_000, transcendentals=0, bytes_accessed=4_000_000),
        name="kv_kernel",
    )(doc_blocks, hidden, norm_gain[None], w_key, w_value, k_gain[None], freq)

    row1 = moved(kv, 1, 0)
    up1 = moved(kv, 0, 1)
    down1 = moved(kv, 0, -1)
    row2 = moved(kv, 2, 0)
    up2 = moved(kv, 0, 2, (0, 1))
    level1 = [row1, up1, down1, row2, up2]

    cols = 512
    queries = pl.pallas_call(
        q_kernel,
        grid=(w_query.shape[1] // cols,),
        out_shape=jax.ShapeDtypeStruct((hq, HD, TOK), BF),
        in_specs=[
            pl.BlockSpec((TOK, d), lambda j: (0, 0)),
            pl.BlockSpec((d, cols), lambda j: (0, j)),
            pl.BlockSpec((1, HD), lambda j: (0, 0)),
            pl.BlockSpec((HD, TOK), lambda j: (0, 0)),
            pl.BlockSpec((HD, TOK), lambda j: (0, 0)),
        ],
        out_specs=pl.BlockSpec((cols // HD, HD, TOK), lambda j: (j, 0, 0)),
        cost_estimate=pl.CostEstimate(flops=2_147_000_000, transcendentals=0, bytes_accessed=10_000_000),
        name="q_kernel",
    )(normed, w_query, q_gain[None], cos, sin)

    level2 = [
        moved(up1, 1, 0),
        moved(down1, 1, 0),
        moved(row1, 0, 2),
        moved(row2, 0, -1, (1, 2, 3)),
        moved(row2, 0, 1, (3,)),
        moved(row2, 0, 2, (2, 3)),
    ]
    m_shape = (2, 2, 1, 8 * BLK)
    acc_shape = (2, 2, HD + EXTRA, 8 * BLK)
    m_part, acc_part = pl.pallas_call(
        functools.partial(attend_kernel, LEVEL1, True, False),
        out_shape=(jax.ShapeDtypeStruct(m_shape, F32), jax.ShapeDtypeStruct(acc_shape, F32)),
        in_specs=[SMEM, VM] + [ANY] * (len(LEVEL1) + 1),
        out_specs=[VM, VM],
        scratch_shapes=[
            pltpu.VMEM((len(LEVEL1) + 1, 2, TOK, 2 * HD), BF),
            pltpu.SMEM((len(LEVEL1),), jnp.int32),
            pltpu.SemaphoreType.DMA((len(LEVEL1) + 1,)),
        ],
        cost_estimate=pl.CostEstimate(flops=6_000_000_000, transcendentals=0, bytes_accessed=6_000_000),
        name="attend_near",
    )(doc_blocks, queries, *level1, kv)
    half = w_out.shape[1] // 2
    send, keep = pl.pallas_call(
        functools.partial(attend_kernel, LEVEL2, False, True),
        out_shape=(
            jax.ShapeDtypeStruct((TOK, half), BF),
            jax.ShapeDtypeStruct((TOK, half), F32),
        ),
        in_specs=[SMEM, VM] + [ANY] * len(LEVEL2) + [VM, VM, ANY],
        out_specs=[VM, VM],
        scratch_shapes=[
            pltpu.VMEM((len(LEVEL2), 2, TOK, 2 * HD), BF),
            pltpu.SMEM((len(LEVEL2),), jnp.int32),
            pltpu.VMEM(m_shape, F32),
            pltpu.VMEM(acc_shape, F32),
            pltpu.VMEM((TOK, hq * HD), BF),
            pltpu.VMEM(w_out.shape, BF),
            pltpu.SemaphoreType.DMA((len(LEVEL2),)),
            pltpu.SemaphoreType.DMA,
        ],
        cost_estimate=pl.CostEstimate(flops=9_000_000_000, transcendentals=0, bytes_accessed=14_000_000),
        name="attend_far",
    )(doc_blocks, queries, *level2, m_part, acc_part, w_out)
    other = lax.ppermute(send, "role", [(0, 1), (1, 0)])
    return (keep + other.astype(F32)).astype(BF)


def solution(mesh):
    return jax.shard_map(
        on_device,
        mesh=mesh,
        in_specs=(
            P("tok", None), P(), P(), P(None, "role"), P(None, "role"), P(None, "role"),
            P(), P(), P("role", None),
        ),
        out_specs=P("tok", "role"),
        check_vma=False,
    )
```

```python
import functools

import numpy as np
import jax
import jax.numpy as jnp
from jax import lax
from jax.experimental import pallas as pl
from jax.experimental.pallas import tpu as pltpu
from jax.sharding import PartitionSpec as P

HD = 128
BLK = 128
MOST = 16
NDOCS = 10
EPSILON = 1e-06
THETA = 1000000.0
TOK = 256
RING = 4
EXTRA = 16
AHEAD = 3
BF = jnp.bfloat16
F32 = jnp.float32
SCALE2 = float(HD ** (-0.5) * np.log2(np.e))


def doc_start(docs, block):
    end = jnp.int32(0)
    start = jnp.int32(0)
    for j in range(NDOCS):
        end = end + docs[j]
        start = jnp.where(end <= block, end, start)
    return start


def head_norm_rope(x, gain, cos, sin):
    ms = jnp.mean(x * x, axis=-1, keepdims=True)
    x = x * lax.rsqrt(ms + EPSILON) * gain
    return (x * cos + pltpu.roll(x, HD // 2, 1) * sin).astype(BF)


def head_norm_rope_t(x, gain, cos, sin):
    ms = jnp.mean(x * x, axis=0, keepdims=True)
    x = x * lax.rsqrt(ms + EPSILON) * gain
    turned = jnp.concatenate([x[HD // 2:], x[:HD // 2]], axis=0)
    return (x * cos + turned * sin).astype(BF)


def kv_kernel(docs, hid, ngain, wk, wv, kgain, freq, normed_o, kv_o, cos_o, sin_o):
    first = lax.axis_index("tok") * 2
    s0 = doc_start(docs, first) * BLK
    s1 = doc_start(docs, first + 1) * BLK
    row = lax.broadcasted_iota(jnp.int32, (TOK, HD), 0)
    pos = first * BLK + row - jnp.where(row < BLK, s0, s1)
    ang = pos.astype(F32) * freq[...]
    cos = jnp.cos(ang)
    lane = lax.broadcasted_iota(jnp.int32, (TOK, HD), 1)
    sin = jnp.sin(ang)
    sin = jnp.where(lane < HD // 2, -sin, sin)
    cos_o[...] = cos.T
    sin_o[...] = sin.T
    x = hid[...].astype(F32)
    ms = jnp.mean(x * x, axis=-1, keepdims=True)
    normed = (x * lax.rsqrt(ms + EPSILON) * ngain[...]).astype(BF)
    normed_o[...] = normed
    k = jnp.dot(normed, wk[...], preferred_element_type=F32)
    for h in range(2):
        kv_o[0, :, h * HD:(h + 1) * HD] = head_norm_rope(
            k[:, h * HD:(h + 1) * HD], kgain[...], cos, sin)
    kv_o[1] = jnp.dot(normed, wv[...], preferred_element_type=F32).T.astype(BF)


def q_kernel(normed, wq, qgain, cos, sin, q_o):
    q = jnp.dot(normed[...], wq[...], preferred_element_type=F32)
    gain = jnp.broadcast_to(qgain[...], (TOK, HD)).T
    for h in range(q.shape[1] // HD):
        q_o[h] = head_norm_rope_t(q[:, h * HD:(h + 1) * HD].T, gain, cos[...], sin[...])


def attend_kernel(table, first_stage, last_stage, *refs):
    slots = len(table)
    refs = list(refs)
    docs, q = refs[:2]
    refs = refs[2:]
    count = slots if first_stage else slots - 1
    pieces, refs = list(refs[:count]), refs[count:]
    me = lax.axis_index("tok")
    role = lax.axis_index("role")
    if first_stage:
        own, refs = refs[0], refs[1:]
    else:
        m_in, acc_in, wout = refs[:3]
        refs = refs[3:]
    if last_stage:
        send_o, keep_o, win, hops, m_s, acc_s, att, wbuf, sems, wsem = refs
        wcopy = pltpu.make_async_copy(wout, wbuf, wsem)
    else:
        m_s, acc_s, win, hops, sems = refs
    if first_stage:
        sources = pieces + [own]
    else:
        sources = pieces[:-1] + [pieces[-1].at[0], pieces[-1].at[1]]
    copies = [pltpu.make_async_copy(p, win.at[n], sems.at[n]) for n, p in enumerate(sources)]
    if not first_stage:
        copies.append(pltpu.make_async_copy(m_in, m_s, sems.at[slots]))
        copies.append(pltpu.make_async_copy(acc_in, acc_s, sems.at[slots + 1]))
    for c in copies:
        c.start()
    if last_stage:
        wcopy.start()
    z = me % RING
    for n, row in enumerate(table):
        hop = jnp.int32(row[0])
        for zz in range(1, RING):
            hop = jnp.where(z == zz, jnp.int32(row[zz]), hop)
        hops[n] = hop
    for c in copies:
        c.wait()
    step = 2 * BLK

    def tile(i, slot, lo, size, mask, first):
        units = [(g, j) for g in range(2) for j in range(4)]

        def scores(g, j):
            k = win[slot, 0, lo:lo + size, g * HD:(g + 1) * HD]
            qt = jnp.concatenate(
                [q[g * 8 + 2 * j + e, :, i * BLK:(i + 1) * BLK] for e in range(2)], axis=1)
            s = jnp.dot(k, qt, preferred_element_type=F32)
            return s if mask is None else jnp.where(mask, s, -1e30)

        ahead = [scores(*units[n]) for n in range(AHEAD)]
        for n, (g, j) in enumerate(units):
            s = ahead.pop(0)
            if n + AHEAD < len(units):
                ahead.append(scores(*units[n + AHEAD]))
            cols = slice(j * step, (j + 1) * step)
            v = win[slot, 1, g * HD:(g + 1) * HD, lo:lo + size]
            v1 = jnp.concatenate([v, jnp.ones((EXTRA, size), BF)], axis=0)
            top = jnp.max(s, axis=0, keepdims=True)
            if first:
                m_new = top
            else:
                m_old = m_s[i, g, :, cols]
                m_new = jnp.maximum(m_old, top)
            p = jnp.exp2((s - m_new) * SCALE2).astype(BF)
            pv = jnp.dot(v1, p, preferred_element_type=F32)
            if first:
                acc_s[i, g, :, cols] = pv
            else:
                acc_s[i, g, :, cols] = acc_s[i, g, :, cols] * jnp.exp2((m_old - m_new) * SCALE2) + pv
            m_s[i, g, :, cols] = m_new

    for i in range(2):
        block = me * 2 + i
        depth = block - doc_start(docs, block)
        if first_stage:
            size = BLK * (i + 1)
            key = lax.broadcasted_iota(jnp.int32, (size, step), 0)
            token = lax.broadcasted_iota(jnp.int32, (size, step), 1) % BLK
            mask = key <= token + i * BLK
            if i == 1:
                mask = mask & (key >= jnp.where(depth == 0, BLK, 0))
            tile(i, slots, 0, size, mask, True)

        @pl.loop(0, slots)
        def _(slot):
            hop = hops[slot]

            @pl.when((hop > 0) & (2 * hop + i <= depth))
            def _():
                tile(i, slot, 0, 2 * BLK, None, False)

            @pl.when((hop > 0) & (2 * hop + i == depth + 1))
            def _():
                tile(i, slot, BLK, BLK, None, False)

        if last_stage:
            for g in range(2):
                for h in range(8):
                    cols = slice(h * BLK, (h + 1) * BLK)
                    o = acc_s[i, g, :HD, cols] * (1.0 / acc_s[i, g, HD:HD + 1, cols])
                    att[i * BLK:(i + 1) * BLK, (g * 8 + h) * HD:(g * 8 + h + 1) * HD] = o.T.astype(BF)
    if last_stage:
        wcopy.wait()
        half = wout.shape[1] // 2
        a = att[...]
        theirs = pl.multiple_of((1 - role) * half, half)
        mine = pl.multiple_of(role * half, half)
        send_o[...] = jnp.dot(a, wbuf[:, pl.ds(theirs, half)], preferred_element_type=F32).astype(BF)
        keep_o[...] = jnp.dot(a, wbuf[:, pl.ds(mine, half)], preferred_element_type=F32)


SMEM = pl.BlockSpec(memory_space=pltpu.MemorySpace.SMEM)
ANY = pl.BlockSpec(memory_space=pl.ANY)
VM = pl.BlockSpec(memory_space=pltpu.MemorySpace.VMEM)


def shifted(value, by):
    peers = lax.axis_size("tok")
    return lax.ppermute(value, "tok", [(t, (t + by) % peers) for t in range(peers)])


def moved(value, rows, turn, senders=(0, 1, 2, 3)):
    peers = lax.axis_size("tok")
    pairs = []
    for t in range(peers):
        z = t % RING
        if z in senders:
            pairs.append((t, (t - z + (z + turn) % RING + rows * RING) % peers))
    return lax.ppermute(value, "tok", pairs)


LEVEL1 = ((4, 4, 4, 4), (1, 1, 1, 1), (0, 0, 0, 3), (8, 8, 8, 8))
LEVEL2 = ((5, 5, 5, 5), (3, 3, 3, 7), (7, 7, 7, 0), (2, 2, 6, 6), (6, 6, 2, 2))


def on_device(hidden, doc_blocks, norm_gain, w_query, w_key, w_value, q_gain, k_gain, w_out):
    d = hidden.shape[1]
    hq = w_query.shape[1] // HD
    freq = THETA ** (-(np.arange(HD // 2, dtype=np.float32) * np.float32(2.0)) / np.float32(HD))
    freq = jnp.asarray(np.concatenate([freq, freq])[None].astype(np.float32))
    normed, kv, cos, sin = pl.pallas_call(
        kv_kernel,
        out_shape=(
            jax.ShapeDtypeStruct((TOK, d), BF),
            jax.ShapeDtypeStruct((2, TOK, 2 * HD), BF),
            jax.ShapeDtypeStruct((HD, TOK), F32),
            jax.ShapeDtypeStruct((HD, TOK), F32),
        ),
        in_specs=[SMEM] + [VM] * 6,
        out_specs=[VM] * 4,
        cost_estimate=pl.CostEstimate(flops=540_000_000, transcendentals=0, bytes_accessed=4_000_000),
        name="kv_kernel",
    )(doc_blocks, hidden, norm_gain[None], w_key, w_value, k_gain[None], freq)

    row1 = shifted(kv, RING)
    row2 = shifted(kv, 2 * RING)
    next1 = shifted(kv, 1)
    down1 = moved(kv, 0, -1)
    level1 = [row1, next1, down1, row2]

    cols = 512
    queries = pl.pallas_call(
        q_kernel,
        grid=(w_query.shape[1] // cols,),
        out_shape=jax.ShapeDtypeStruct((hq, HD, TOK), BF),
        in_specs=[
            pl.BlockSpec((TOK, d), lambda j: (0, 0)),
            pl.BlockSpec((d, cols), lambda j: (0, j)),
            pl.BlockSpec((1, HD), lambda j: (0, 0)),
            pl.BlockSpec((HD, TOK), lambda j: (0, 0)),
            pl.BlockSpec((HD, TOK), lambda j: (0, 0)),
        ],
        out_specs=pl.BlockSpec((cols // HD, HD, TOK), lambda j: (j, 0, 0)),
        cost_estimate=pl.CostEstimate(flops=2_147_000_000, transcendentals=0, bytes_accessed=10_000_000),
        name="q_kernel",
    )(normed, w_query, q_gain[None], cos, sin)

    lower = lax.axis_index("tok") % RING < RING // 2
    pair = jnp.stack([row1, jnp.where(lower, kv, row2)])
    level2 = [
        shifted(next1, RING),
        shifted(down1, RING),
        moved(row2, 0, -1, (1, 2, 3)),
        moved(pair, 0, 2),
    ]
    m_shape = (2, 2, 1, 8 * BLK)
    acc_shape = (2, 2, HD + EXTRA, 8 * BLK)
    m_part, acc_part = pl.pallas_call(
        functools.partial(attend_kernel, LEVEL1, True, False),
        out_shape=(jax.ShapeDtypeStruct(m_shape, F32), jax.ShapeDtypeStruct(acc_shape, F32)),
        in_specs=[SMEM, VM] + [ANY] * (len(LEVEL1) + 1),
        out_specs=[VM, VM],
        scratch_shapes=[
            pltpu.VMEM((len(LEVEL1) + 1, 2, TOK, 2 * HD), BF),
            pltpu.SMEM((len(LEVEL1),), jnp.int32),
            pltpu.SemaphoreType.DMA((len(LEVEL1) + 1,)),
        ],
        cost_estimate=pl.CostEstimate(flops=6_000_000_000, transcendentals=0, bytes_accessed=6_000_000),
        name="attend_near",
    )(doc_blocks, queries, *level1, kv)
    half = w_out.shape[1] // 2
    send, keep = pl.pallas_call(
        functools.partial(attend_kernel, LEVEL2, False, True),
        out_shape=(
            jax.ShapeDtypeStruct((TOK, half), BF),
            jax.ShapeDtypeStruct((TOK, half), F32),
        ),
        in_specs=[SMEM, VM] + [ANY] * (len(level2) + 3),
        out_specs=[VM, VM],
        scratch_shapes=[
            pltpu.VMEM((len(LEVEL2), 2, TOK, 2 * HD), BF),
            pltpu.SMEM((len(LEVEL2),), jnp.int32),
            pltpu.VMEM(m_shape, F32),
            pltpu.VMEM(acc_shape, F32),
            pltpu.VMEM((TOK, hq * HD), BF),
            pltpu.VMEM(w_out.shape, BF),
            pltpu.SemaphoreType.DMA((len(LEVEL2) + 2,)),
            pltpu.SemaphoreType.DMA,
        ],
        cost_estimate=pl.CostEstimate(flops=9_000_000_000, transcendentals=0, bytes_accessed=14_000_000),
        name="attend_far",
    )(doc_blocks, queries, *level2, m_part, acc_part, w_out)
    other = lax.ppermute(send, "role", [(0, 1), (1, 0)])
    return (keep + other.astype(F32)).astype(BF)


def solution(mesh):
    return jax.shard_map(
        on_device,
        mesh=mesh,
        in_specs=(
            P("tok", None), P(), P(), P(None, "role"), P(None, "role"), P(None, "role"),
            P(), P(), P("role", None),
        ),
        out_specs=P("tok", "role"),
        check_vma=False,
    )
```

```python
import functools

import numpy as np
import jax
import jax.numpy as jnp
from jax import lax
from jax.experimental import pallas as pl
from jax.experimental.pallas import tpu as pltpu
from jax.sharding import PartitionSpec as P

HD = 128
BLK = 128
MOST = 16
NDOCS = 10
EPSILON = 1e-06
THETA = 1000000.0
TOK = 256
RING = 4
EXTRA = 16
AHEAD = 3
BF = jnp.bfloat16
F32 = jnp.float32
SCALE2 = float(HD ** (-0.5) * np.log2(np.e))


def doc_start(docs, block):
    end = jnp.int32(0)
    start = jnp.int32(0)
    for j in range(NDOCS):
        end = end + docs[j]
        start = jnp.where(end <= block, end, start)
    return start


def head_norm_rope(x, gain, cos, sin):
    ms = jnp.mean(x * x, axis=-1, keepdims=True)
    x = x * lax.rsqrt(ms + EPSILON) * gain
    return (x * cos + pltpu.roll(x, HD // 2, 1) * sin).astype(BF)


def head_norm_rope_t(x, gain, cos, sin):
    ms = jnp.mean(x * x, axis=0, keepdims=True)
    x = x * lax.rsqrt(ms + EPSILON) * gain
    turned = jnp.concatenate([x[HD // 2:], x[:HD // 2]], axis=0)
    return (x * cos + turned * sin).astype(BF)


def fetch(pairs, sems):
    copies = [pltpu.make_async_copy(src, dst, sems.at[n]) for n, (src, dst) in enumerate(pairs)]
    for c in copies:
        c.start()
    return copies


def kv_kernel(docs, hid, ngain, wk, wv, kgain, freq, normed_o, kv_o, cos_o, sin_o,
              hid_b, ngain_b, wk_b, wv_b, kgain_b, freq_b, sems):
    copies = fetch(((freq, freq_b), (ngain, ngain_b), (kgain, kgain_b), (hid, hid_b),
                    (wk, wk_b), (wv, wv_b)), sems)
    first = lax.axis_index("tok") * 2
    s0 = doc_start(docs, first) * BLK
    s1 = doc_start(docs, first + 1) * BLK
    row = lax.broadcasted_iota(jnp.int32, (TOK, HD), 0)
    pos = first * BLK + row - jnp.where(row < BLK, s0, s1)
    for c in copies[:3]:
        c.wait()
    ang = pos.astype(F32) * freq_b[...]
    cos = jnp.cos(ang)
    lane = lax.broadcasted_iota(jnp.int32, (TOK, HD), 1)
    sin = jnp.sin(ang)
    sin = jnp.where(lane < HD // 2, -sin, sin)
    cos_o[...] = cos.T
    sin_o[...] = sin.T
    copies[3].wait()
    x = hid_b[...].astype(F32)
    ms = jnp.mean(x * x, axis=-1, keepdims=True)
    normed = (x * lax.rsqrt(ms + EPSILON) * ngain_b[...]).astype(BF)
    normed_o[...] = normed
    copies[4].wait()
    k = jnp.dot(normed, wk_b[...], preferred_element_type=F32)
    copies[5].wait()
    v = jnp.dot(normed, wv_b[...], preferred_element_type=F32)
    for h in range(2):
        kv_o[0, :, h * HD:(h + 1) * HD] = head_norm_rope(
            k[:, h * HD:(h + 1) * HD], kgain_b[...], cos, sin)
    kv_o[1] = v.T.astype(BF)


def q_kernel(normed, wq, qgain, cos, sin, q_o, qgain_b, sems):
    copies = fetch([(qgain, qgain_b)], sems)
    copies[0].wait()
    gain = jnp.broadcast_to(qgain_b[...], (TOK, HD)).T
    width = 2 * HD
    for b in range(wq.shape[1] // width):
        q = jnp.dot(normed[...], wq[:, b * width:(b + 1) * width], preferred_element_type=F32)
        for h in range(2):
            q_o[2 * b + h] = head_norm_rope_t(
                q[:, h * HD:(h + 1) * HD].T, gain, cos[...], sin[...])


def attend_kernel(table, first_stage, last_stage, *refs):
    slots = len(table)
    refs = list(refs)
    docs, q = refs[:2]
    refs = refs[2:]
    pieces, refs = list(refs[:slots]), refs[slots:]
    me = lax.axis_index("tok")
    role = lax.axis_index("role")
    if first_stage:
        own, refs = refs[0], refs[1:]
    else:
        m_in, acc_in = refs[:2]
        refs = refs[2:]
    if last_stage:
        wout, refs = refs[0], refs[1:]
        send_o, keep_o, win, hops, m_s, acc_s, att = refs
    else:
        m_s, acc_s, win, hops = refs
    sources = pieces + ([own] if first_stage else [])
    for n, piece in enumerate(sources):
        win[n] = piece[...]
    if not first_stage:
        m_s[...] = m_in[...]
        acc_s[...] = acc_in[...]
    z = me % RING
    for n, row in enumerate(table):
        hop = jnp.int32(row[0])
        for zz in range(1, RING):
            hop = jnp.where(z == zz, jnp.int32(row[zz]), hop)
        hops[n] = hop
    step = 2 * BLK

    def tile(i, slot, lo, size, mask, first):
        units = [(g, j) for g in range(2) for j in range(4)]

        def scores(g, j):
            k = win[slot, 0, lo:lo + size, g * HD:(g + 1) * HD]
            qt = jnp.concatenate(
                [q[g * 8 + 2 * j + e, :, i * BLK:(i + 1) * BLK] for e in range(2)], axis=1)
            s = jnp.dot(k, qt, preferred_element_type=F32)
            return s if mask is None else jnp.where(mask, s, -1e30)

        ahead = [scores(*units[n]) for n in range(AHEAD)]
        for n, (g, j) in enumerate(units):
            s = ahead.pop(0)
            if n + AHEAD < len(units):
                ahead.append(scores(*units[n + AHEAD]))
            cols = slice(j * step, (j + 1) * step)
            v = win[slot, 1, g * HD:(g + 1) * HD, lo:lo + size]
            v1 = jnp.concatenate([v, jnp.ones((EXTRA, size), BF)], axis=0)
            top = jnp.max(s, axis=0, keepdims=True)
            if first:
                m_new = top
            else:
                m_old = m_s[i, g, :, cols]
                m_new = jnp.maximum(m_old, top)
            p = jnp.exp2((s - m_new) * SCALE2).astype(BF)
            pv = jnp.dot(v1, p, preferred_element_type=F32)
            if first:
                acc_s[i, g, :, cols] = pv
            else:
                acc_s[i, g, :, cols] = acc_s[i, g, :, cols] * jnp.exp2((m_old - m_new) * SCALE2) + pv
            m_s[i, g, :, cols] = m_new

    for i in range(2):
        block = me * 2 + i
        depth = block - doc_start(docs, block)
        if first_stage:
            size = BLK * (i + 1)
            key = lax.broadcasted_iota(jnp.int32, (size, step), 0)
            token = lax.broadcasted_iota(jnp.int32, (size, step), 1) % BLK
            mask = key <= token + i * BLK
            if i == 1:
                mask = mask & (key >= jnp.where(depth == 0, BLK, 0))
            tile(i, slots, 0, size, mask, True)

        @pl.loop(0, slots)
        def _(slot):
            hop = hops[slot]

            @pl.when((hop > 0) & (2 * hop + i <= depth))
            def _():
                tile(i, slot, 0, 2 * BLK, None, False)

            @pl.when((hop > 0) & (2 * hop + i == depth + 1))
            def _():
                tile(i, slot, BLK, BLK, None, False)

        if last_stage:
            for g in range(2):
                for h in range(8):
                    cols = slice(h * BLK, (h + 1) * BLK)
                    o = acc_s[i, g, :HD, cols] * (1.0 / acc_s[i, g, HD:HD + 1, cols])
                    att[i * BLK:(i + 1) * BLK, (g * 8 + h) * HD:(g * 8 + h + 1) * HD] = o.T.astype(BF)
    if last_stage:
        half = wout.shape[1] // 2
        a = att[...]
        theirs = pl.multiple_of((1 - role) * half, half)
        mine = pl.multiple_of(role * half, half)
        send_o[...] = jnp.dot(a, wout[:, pl.ds(theirs, half)], preferred_element_type=F32).astype(BF)
        keep_o[...] = jnp.dot(a, wout[:, pl.ds(mine, half)], preferred_element_type=F32)


HBM = pl.BlockSpec(memory_space=pltpu.MemorySpace.HBM)
SMEM = pl.BlockSpec(memory_space=pltpu.MemorySpace.SMEM)
VM = pl.BlockSpec(memory_space=pltpu.MemorySpace.VMEM)


def shifted(value, by):
    peers = lax.axis_size("tok")
    return lax.ppermute(value, "tok", [(t, (t + by) % peers) for t in range(peers)])


def moved(value, rows, turn, senders=(0, 1, 2, 3)):
    peers = lax.axis_size("tok")
    pairs = []
    for t in range(peers):
        z = t % RING
        if z in senders:
            pairs.append((t, (t - z + (z + turn) % RING + rows * RING) % peers))
    return lax.ppermute(value, "tok", pairs)


NEAR = ((4, 4, 4, 4), (0, 1, 1, 1), (0, 0, 0, 3), (8, 8, 8, 8))
MID = ((1, 5, 5, 5), (3, 3, 3, 7), (2, 2, 6, 6))
FAR = ((6, 6, 2, 2), (7, 7, 7, 0), (5, 0, 0, 0))


def on_device(hidden, doc_blocks, norm_gain, w_query, w_key, w_value, q_gain, k_gain, w_out):
    d = hidden.shape[1]
    hq = w_query.shape[1] // HD
    freq = THETA ** (-(np.arange(HD // 2, dtype=np.float32) * np.float32(2.0)) / np.float32(HD))
    freq = jnp.asarray(np.concatenate([freq, freq])[None].astype(np.float32))
    doc_blocks, hidden, norm_row, w_key, w_value, k_row, freq, q_row = (
        pltpu.with_memory_space_constraint(x, pltpu.MemorySpace.HBM)
        for x in (doc_blocks, hidden, norm_gain[None], w_key, w_value, k_gain[None], freq, q_gain[None]))
    normed, kv, cos, sin = pl.pallas_call(
        kv_kernel,
        out_shape=(
            jax.ShapeDtypeStruct((TOK, d), BF),
            jax.ShapeDtypeStruct((2, TOK, 2 * HD), BF),
            jax.ShapeDtypeStruct((HD, TOK), F32),
            jax.ShapeDtypeStruct((HD, TOK), F32),
        ),
        in_specs=[SMEM] + [HBM] * 6,
        out_specs=[VM] * 4,
        scratch_shapes=[
            pltpu.VMEM((TOK, d), BF),
            pltpu.VMEM((1, d), F32),
            pltpu.VMEM(w_key.shape, BF),
            pltpu.VMEM(w_value.shape, BF),
            pltpu.VMEM((1, HD), F32),
            pltpu.VMEM((1, HD), F32),
            pltpu.SemaphoreType.DMA((6,)),
        ],
        cost_estimate=pl.CostEstimate(flops=8_000_000_000, transcendentals=0, bytes_accessed=40_000_000),
        name="kv_kernel",
        compiler_params=pltpu.CompilerParams(vmem_limit_bytes=16 << 20),
    )(doc_blocks, hidden, norm_row, w_key, w_value, k_row, freq)

    row1 = shifted(kv, RING)
    up1 = moved(kv, 0, 1)
    down1 = moved(kv, 0, -1)
    row2 = shifted(kv, 2 * RING)

    queries = pl.pallas_call(
        q_kernel,
        out_shape=jax.ShapeDtypeStruct((hq, HD, TOK), BF),
        in_specs=[VM, VM, HBM, VM, VM],
        out_specs=VM,
        scratch_shapes=[
            pltpu.VMEM((1, HD), F32),
            pltpu.SemaphoreType.DMA((1,)),
        ],
        cost_estimate=pl.CostEstimate(flops=2_147_000_000, transcendentals=0, bytes_accessed=10_000_000),
        name="q_kernel",
        compiler_params=pltpu.CompilerParams(vmem_limit_bytes=24 << 20),
    )(normed, w_query, q_row, cos, sin)

    lower = lax.axis_index("tok") % RING < RING // 2
    mid = [shifted(up1, RING), shifted(down1, RING), moved(row1, 0, 2)]
    far = [
        moved(jnp.where(lower, kv, row2), 0, 2),
        moved(row2, 0, -1, (1, 2, 3)),
        moved(row2, 0, 1, (3,)),
    ]
    state = (
        jax.ShapeDtypeStruct((2, 2, 1, 8 * BLK), F32),
        jax.ShapeDtypeStruct((2, 2, HD + EXTRA, 8 * BLK), F32),
    )

    def stage(table, name, operands, extra):
        return pl.pallas_call(
            functools.partial(attend_kernel, table, extra, False),
            out_shape=state,
            in_specs=[SMEM] + [VM] * (len(operands) + 1),
            out_specs=[VM, VM],
            scratch_shapes=[
                pltpu.VMEM((len(table) + extra, 2, TOK, 2 * HD), BF),
                pltpu.SMEM((len(table),), jnp.int32),
            ],
            cost_estimate=pl.CostEstimate(flops=6_000_000_000, transcendentals=0, bytes_accessed=6_000_000),
            name=name,
            compiler_params=pltpu.CompilerParams(vmem_limit_bytes=24 << 20),
        )(doc_blocks, queries, *operands)

    partial = stage(NEAR, "attend_near", [row1, up1, down1, row2, kv], True)
    partial = stage(MID, "attend_mid", [*mid, *partial], False)
    half = w_out.shape[1] // 2
    send, keep = pl.pallas_call(
        functools.partial(attend_kernel, FAR, False, True),
        out_shape=(
            jax.ShapeDtypeStruct((TOK, half), BF),
            jax.ShapeDtypeStruct((TOK, half), F32),
        ),
        in_specs=[SMEM] + [VM] * (len(FAR) + 4),
        out_specs=[VM, VM],
        scratch_shapes=[
            pltpu.VMEM((len(FAR), 2, TOK, 2 * HD), BF),
            pltpu.SMEM((len(FAR),), jnp.int32),
            pltpu.VMEM(state[0].shape, F32),
            pltpu.VMEM(state[1].shape, F32),
            pltpu.VMEM((TOK, hq * HD), BF),
        ],
        cost_estimate=pl.CostEstimate(flops=9_000_000_000, transcendentals=0, bytes_accessed=14_000_000),
        name="attend_far",
        compiler_params=pltpu.CompilerParams(vmem_limit_bytes=28 << 20),
    )(doc_blocks, queries, *far, *partial, w_out)
    other = lax.ppermute(send, "role", [(0, 1), (1, 0)])
    return (keep + other.astype(F32)).astype(BF)


def solution(mesh):
    return jax.shard_map(
        on_device,
        mesh=mesh,
        in_specs=(
            P("tok", None), P(), P(), P(None, "role"), P(None, "role"), P(None, "role"),
            P(), P(), P("role", None),
        ),
        out_specs=P("tok", "role"),
        check_vma=False,
    )
```

```python
import functools

import numpy as np
import jax
import jax.numpy as jnp
from jax import lax
from jax.experimental import pallas as pl
from jax.experimental.pallas import tpu as pltpu
from jax.sharding import PartitionSpec as P

HD = 128
BLK = 128
NDOCS = 10
EPSILON = 1e-06
THETA = 1000000.0
TOK = 256
RING = 4
EXTRA = 16
AHEAD = 3
QBLOCKS = 8
BF = jnp.bfloat16
F32 = jnp.float32
SCALE2 = float(HD ** (-0.5) * np.log2(np.e))


def doc_start(docs, block):
    end = jnp.int32(0)
    start = jnp.int32(0)
    for j in range(NDOCS):
        end = end + docs[j]
        start = jnp.where(end <= block, end, start)
    return start


def head_norm_rope(x, gain, cos, sin):
    ms = jnp.mean(x * x, axis=-1, keepdims=True)
    x = x * lax.rsqrt(ms + EPSILON) * gain
    return (x * cos + pltpu.roll(x, HD // 2, 1) * sin).astype(BF)


def head_norm_rope_t(x, gain, cos, sin):
    ms = jnp.mean(x * x, axis=0, keepdims=True)
    x = x * lax.rsqrt(ms + EPSILON) * gain
    turned = jnp.concatenate([x[HD // 2:], x[:HD // 2]], axis=0)
    return (x * cos + turned * sin).astype(BF)


def fetch(pairs, sems):
    copies = [pltpu.make_async_copy(src, dst, sems.at[n]) for n, (src, dst) in enumerate(pairs)]
    for c in copies:
        c.start()
    return copies


def kv_kernel(docs, hid, ngain, wk, wv, kgain, freq, normed_o, kv_o, cos_o, sin_o,
              hid_b, ngain_b, wk_b, wv_b, kgain_b, freq_b, sems):
    copies = fetch(((freq, freq_b), (ngain, ngain_b), (kgain, kgain_b), (hid, hid_b),
                    (wk, wk_b), (wv, wv_b)), sems)
    first = lax.axis_index("tok") * 2
    s0 = doc_start(docs, first) * BLK
    s1 = doc_start(docs, first + 1) * BLK
    row = lax.broadcasted_iota(jnp.int32, (TOK, HD), 0)
    pos = first * BLK + row - jnp.where(row < BLK, s0, s1)
    for c in copies[:3]:
        c.wait()
    ang = pos.astype(F32) * freq_b[...]
    cos = jnp.cos(ang)
    lane = lax.broadcasted_iota(jnp.int32, (TOK, HD), 1)
    sin = jnp.sin(ang)
    sin = jnp.where(lane < HD // 2, -sin, sin)
    cos_o[...] = cos.T
    sin_o[...] = sin.T
    copies[3].wait()
    x = hid_b[...].astype(F32)
    ms = jnp.mean(x * x, axis=-1, keepdims=True)
    normed = (x * lax.rsqrt(ms + EPSILON) * ngain_b[...]).astype(BF)
    normed_o[...] = normed
    copies[4].wait()
    k = jnp.dot(normed, wk_b[...], preferred_element_type=F32)
    copies[5].wait()
    v = jnp.dot(normed, wv_b[...], preferred_element_type=F32)
    for h in range(2):
        kv_o[0, :, h * HD:(h + 1) * HD] = head_norm_rope(
            k[:, h * HD:(h + 1) * HD], kgain_b[...], cos, sin)
    kv_o[1] = v.T.astype(BF)


def q_kernel(normed, wq, qgain, cos, sin, q_o, wq_b, acc, qgain_b, sems):
    depth = wq.shape[0]
    rows = depth // QBLOCKS
    copies = fetch([(qgain, qgain_b)] + [
        (wq.at[b * rows:(b + 1) * rows], wq_b.at[b * rows:(b + 1) * rows])
        for b in range(QBLOCKS)], sems)
    half = depth // 2
    width = 2 * HD
    blocks = wq.shape[1] // width
    for c in copies[:1 + QBLOCKS // 2]:
        c.wait()
    gain = jnp.broadcast_to(qgain_b[...], (TOK, HD)).T
    for b in range(blocks):
        cols = slice(b * width, (b + 1) * width)
        acc[:, cols] = jnp.dot(normed[:, :half], wq_b[:half, cols], preferred_element_type=F32)
    for c in copies[1 + QBLOCKS // 2:]:
        c.wait()
    for b in range(blocks):
        cols = slice(b * width, (b + 1) * width)
        q = acc[:, cols] + jnp.dot(normed[:, half:], wq_b[half:, cols], preferred_element_type=F32)
        for h in range(2):
            q_o[2 * b + h] = head_norm_rope_t(
                q[:, h * HD:(h + 1) * HD].T, gain, cos[...], sin[...])


def attend_kernel(table, first_stage, last_stage, *refs):
    slots = len(table)
    refs = list(refs)
    docs, q = refs[:2]
    refs = refs[2:]
    pieces, refs = list(refs[:slots]), refs[slots:]
    me = lax.axis_index("tok")
    role = lax.axis_index("role")
    if first_stage:
        own, refs = refs[0], refs[1:]
    else:
        m_in, acc_in = refs[:2]
        refs = refs[2:]
    if last_stage:
        wout, refs = refs[0], refs[1:]
        send_o, keep_o, win, hops, m_s, acc_s, att = refs
    else:
        m_s, acc_s, win, hops = refs
    sources = pieces + ([own] if first_stage else [])
    for n, piece in enumerate(sources):
        win[n] = piece[...]
    if not first_stage:
        m_s[...] = m_in[...]
        acc_s[...] = acc_in[...]
    z = me % RING
    for n, row in enumerate(table):
        hop = jnp.int32(row[0])
        for zz in range(1, RING):
            hop = jnp.where(z == zz, jnp.int32(row[zz]), hop)
        hops[n] = hop
    step = 2 * BLK

    def tile(i, slot, lo, size, mask, first):
        units = [(g, j) for g in range(2) for j in range(4)]

        def scores(g, j):
            k = win[slot, 0, lo:lo + size, g * HD:(g + 1) * HD]
            qt = jnp.concatenate(
                [q[g * 8 + 2 * j + e, :, i * BLK:(i + 1) * BLK] for e in range(2)], axis=1)
            s = jnp.dot(k, qt, preferred_element_type=F32)
            return s if mask is None else jnp.where(mask, s, -1e30)

        ahead = [scores(*units[n]) for n in range(AHEAD)]
        for n, (g, j) in enumerate(units):
            s = ahead.pop(0)
            if n + AHEAD < len(units):
                ahead.append(scores(*units[n + AHEAD]))
            cols = slice(j * step, (j + 1) * step)
            v = win[slot, 1, g * HD:(g + 1) * HD, lo:lo + size]
            v1 = jnp.concatenate([v, jnp.ones((EXTRA, size), BF)], axis=0)
            top = jnp.max(s, axis=0, keepdims=True)
            if first:
                m_new = top
            else:
                m_old = m_s[i, g, :, cols]
                m_new = jnp.maximum(m_old, top)
            p = jnp.exp2((s - m_new) * SCALE2).astype(BF)
            pv = jnp.dot(v1, p, preferred_element_type=F32)
            if first:
                acc_s[i, g, :, cols] = pv
            else:
                acc_s[i, g, :, cols] = acc_s[i, g, :, cols] * jnp.exp2((m_old - m_new) * SCALE2) + pv
            m_s[i, g, :, cols] = m_new

    for i in range(2):
        block = me * 2 + i
        depth = block - doc_start(docs, block)
        if first_stage:
            size = BLK * (i + 1)
            key = lax.broadcasted_iota(jnp.int32, (size, step), 0)
            token = lax.broadcasted_iota(jnp.int32, (size, step), 1) % BLK
            mask = key <= token + i * BLK
            if i == 1:
                mask = mask & (key >= jnp.where(depth == 0, BLK, 0))
            tile(i, slots, 0, size, mask, True)

        @pl.loop(0, slots)
        def _(slot):
            hop = hops[slot]

            @pl.when((hop > 0) & (2 * hop + i <= depth))
            def _():
                tile(i, slot, 0, 2 * BLK, None, False)

            @pl.when((hop > 0) & (2 * hop + i == depth + 1))
            def _():
                tile(i, slot, BLK, BLK, None, False)

        if last_stage:
            for g in range(2):
                for h in range(8):
                    cols = slice(h * BLK, (h + 1) * BLK)
                    o = acc_s[i, g, :HD, cols] * (1.0 / acc_s[i, g, HD:HD + 1, cols])
                    att[i * BLK:(i + 1) * BLK, (g * 8 + h) * HD:(g * 8 + h + 1) * HD] = o.T.astype(BF)
    if last_stage:
        half = wout.shape[1] // 2
        a = att[...]
        theirs = pl.multiple_of((1 - role) * half, half)
        mine = pl.multiple_of(role * half, half)
        send_o[...] = jnp.dot(a, wout[:, pl.ds(theirs, half)], preferred_element_type=F32).astype(BF)
        keep_o[...] = jnp.dot(a, wout[:, pl.ds(mine, half)], preferred_element_type=F32)


HBM = pl.BlockSpec(memory_space=pltpu.MemorySpace.HBM)
SMEM = pl.BlockSpec(memory_space=pltpu.MemorySpace.SMEM)
VM = pl.BlockSpec(memory_space=pltpu.MemorySpace.VMEM)


def shifted(value, by):
    peers = lax.axis_size("tok")
    return lax.ppermute(value, "tok", [(t, (t + by) % peers) for t in range(peers)])


def moved(value, rows, turn, senders=(0, 1, 2, 3)):
    peers = lax.axis_size("tok")
    pairs = []
    for t in range(peers):
        z = t % RING
        if z in senders:
            pairs.append((t, (t - z + (z + turn) % RING + rows * RING) % peers))
    return lax.ppermute(value, "tok", pairs)


NEAR = ((4, 4, 4, 4), (0, 1, 1, 1), (0, 0, 0, 3), (8, 8, 8, 8))
MID = ((1, 5, 5, 5), (3, 3, 3, 7), (2, 2, 6, 6))
FAR = ((6, 6, 2, 2), (7, 7, 7, 0), (5, 0, 0, 0))


def layer(hidden, doc_blocks, norm_gain, w_query, w_key, w_value, q_gain, k_gain, w_out):
    d = hidden.shape[1]
    hq = w_query.shape[1] // HD
    freq = THETA ** (-(np.arange(HD // 2, dtype=np.float32) * np.float32(2.0)) / np.float32(HD))
    freq = jnp.asarray(np.concatenate([freq, freq])[None].astype(np.float32))
    doc_blocks, hidden, norm_row, w_key, w_value, k_row, freq, q_row, w_query = (
        pltpu.with_memory_space_constraint(x, pltpu.MemorySpace.HBM)
        for x in (doc_blocks, hidden, norm_gain[None], w_key, w_value, k_gain[None], freq, q_gain[None], w_query))
    normed, kv, cos, sin = pl.pallas_call(
        kv_kernel,
        out_shape=(
            jax.ShapeDtypeStruct((TOK, d), BF),
            jax.ShapeDtypeStruct((2, TOK, 2 * HD), BF),
            jax.ShapeDtypeStruct((HD, TOK), F32),
            jax.ShapeDtypeStruct((HD, TOK), F32),
        ),
        in_specs=[SMEM] + [HBM] * 6,
        out_specs=[VM] * 4,
        scratch_shapes=[
            pltpu.VMEM((TOK, d), BF),
            pltpu.VMEM((1, d), F32),
            pltpu.VMEM(w_key.shape, BF),
            pltpu.VMEM(w_value.shape, BF),
            pltpu.VMEM((1, HD), F32),
            pltpu.VMEM((1, HD), F32),
            pltpu.SemaphoreType.DMA((6,)),
        ],
        cost_estimate=pl.CostEstimate(flops=540_000_000, transcendentals=0, bytes_accessed=4_000_000),
        name="kv_kernel",
        compiler_params=pltpu.CompilerParams(vmem_limit_bytes=16 << 20),
    )(doc_blocks, hidden, norm_row, w_key, w_value, k_row, freq)

    row1 = shifted(kv, RING)
    up1 = moved(kv, 0, 1)
    down1 = moved(kv, 0, -1)
    row2 = shifted(kv, 2 * RING)

    queries = pl.pallas_call(
        q_kernel,
        out_shape=jax.ShapeDtypeStruct((hq, HD, TOK), BF),
        in_specs=[VM, HBM, HBM, VM, VM],
        out_specs=VM,
        scratch_shapes=[
            pltpu.VMEM(w_query.shape, BF),
            pltpu.VMEM((TOK, w_query.shape[1]), F32),
            pltpu.VMEM((1, HD), F32),
            pltpu.SemaphoreType.DMA((QBLOCKS + 1,)),
        ],
        cost_estimate=pl.CostEstimate(flops=2_147_000_000, transcendentals=0, bytes_accessed=10_000_000),
        name="q_kernel",
        compiler_params=pltpu.CompilerParams(vmem_limit_bytes=24 << 20),
    )(normed, w_query, q_row, cos, sin)

    lower = lax.axis_index("tok") % RING < RING // 2
    mid = [shifted(up1, RING)]
    mid.append(shifted(down1, RING))
    mid.append(moved(row1, 0, 2))
    mixed = jnp.where(lower, kv, row2)
    far = [moved(mixed, 0, 2)]
    far.append(moved(row2, 0, -1, (1, 2, 3)))
    far.append(moved(row2, 0, 1, (3,)))
    state = (
        jax.ShapeDtypeStruct((2, 2, 1, 8 * BLK), F32),
        jax.ShapeDtypeStruct((2, 2, HD + EXTRA, 8 * BLK), F32),
    )

    def stage(table, operands, extra):
        return pl.pallas_call(
            functools.partial(attend_kernel, table, extra, False),
            out_shape=state,
            in_specs=[SMEM] + [VM] * (len(operands) + 1),
            out_specs=[VM, VM],
            scratch_shapes=[
                pltpu.VMEM((len(table) + extra, 2, TOK, 2 * HD), BF),
                pltpu.SMEM((len(table),), jnp.int32),
            ],
            cost_estimate=pl.CostEstimate(flops=6_000_000_000, transcendentals=0, bytes_accessed=6_000_000),
            compiler_params=pltpu.CompilerParams(vmem_limit_bytes=24 << 20),
        )(doc_blocks, queries, *operands)

    partial = stage(NEAR, [row1, up1, down1, row2, kv], True)
    partial = stage(MID, [*mid, *partial], False)
    half = w_out.shape[1] // 2
    send, keep = pl.pallas_call(
        functools.partial(attend_kernel, FAR, False, True),
        out_shape=(
            jax.ShapeDtypeStruct((TOK, half), BF),
            jax.ShapeDtypeStruct((TOK, half), F32),
        ),
        in_specs=[SMEM] + [VM] * (len(FAR) + 4),
        out_specs=[VM, VM],
        scratch_shapes=[
            pltpu.VMEM((len(FAR), 2, TOK, 2 * HD), BF),
            pltpu.SMEM((len(FAR),), jnp.int32),
            pltpu.VMEM(state[0].shape, F32),
            pltpu.VMEM(state[1].shape, F32),
            pltpu.VMEM((TOK, hq * HD), BF),
        ],
        cost_estimate=pl.CostEstimate(flops=9_000_000_000, transcendentals=0, bytes_accessed=14_000_000),
        name="attend_far",
        compiler_params=pltpu.CompilerParams(vmem_limit_bytes=28 << 20),
    )(doc_blocks, queries, *far, *partial, w_out)
    other = lax.ppermute(send, "role", [(0, 1), (1, 0)])
    return (keep + other.astype(F32)).astype(BF)


def solution(mesh):
    return jax.shard_map(
        layer,
        mesh=mesh,
        in_specs=(
            P("tok", None), P(), P(), P(None, "role"), P(None, "role"), P(None, "role"),
            P(), P(), P("role", None),
        ),
        out_specs=P("tok", "role"),
        check_vma=False,
    )
```

```python
import functools

import numpy as np
import jax
import jax.numpy as jnp
from jax import lax
from jax.experimental import pallas as pl
from jax.experimental.pallas import tpu as pltpu
from jax.sharding import PartitionSpec as P

HD = 128
BLK = 128
NDOCS = 10
EPSILON = 1e-06
THETA = 1000000.0
TOK = 256
RING = 4
EXTRA = 16
AHEAD = 3
QBLOCKS = 8
BF = jnp.bfloat16
F32 = jnp.float32
SCALE2 = float(HD ** (-0.5) * np.log2(np.e))


def doc_start(docs, block):
    end = jnp.int32(0)
    start = jnp.int32(0)
    for j in range(NDOCS):
        end = end + docs[j]
        start = jnp.where(end <= block, end, start)
    return start


def head_norm_rope(x, gain, cos, sin):
    ms = jnp.mean(x * x, axis=-1, keepdims=True)
    x = x * lax.rsqrt(ms + EPSILON) * gain
    return (x * cos + pltpu.roll(x, HD // 2, 1) * sin).astype(BF)


def head_norm_rope_t(x, gain, cos, sin):
    ms = jnp.mean(x * x, axis=0, keepdims=True)
    x = x * lax.rsqrt(ms + EPSILON) * gain
    turned = jnp.concatenate([x[HD // 2:], x[:HD // 2]], axis=0)
    return (x * cos + turned * sin).astype(BF)


def fetch(pairs, sems):
    copies = [pltpu.make_async_copy(src, dst, sems.at[n]) for n, (src, dst) in enumerate(pairs)]
    for c in copies:
        c.start()
    return copies


def kv_kernel(docs, hid, ngain, wk, wv, kgain, freq, normed_o, kv_o, cos_o, sin_o,
              hid_b, ngain_b, wk_b, wv_b, kgain_b, freq_b, sems):
    copies = fetch(((freq, freq_b), (ngain, ngain_b), (kgain, kgain_b), (hid, hid_b),
                    (wk, wk_b), (wv, wv_b)), sems)
    first = lax.axis_index("tok") * 2
    s0 = doc_start(docs, first) * BLK
    s1 = doc_start(docs, first + 1) * BLK
    row = lax.broadcasted_iota(jnp.int32, (TOK, HD), 0)
    pos = first * BLK + row - jnp.where(row < BLK, s0, s1)
    for c in copies[:3]:
        c.wait()
    ang = pos.astype(F32) * freq_b[...]
    cos = jnp.cos(ang)
    lane = lax.broadcasted_iota(jnp.int32, (TOK, HD), 1)
    sin = jnp.sin(ang)
    sin = jnp.where(lane < HD // 2, -sin, sin)
    cos_o[...] = cos.T
    sin_o[...] = sin.T
    copies[3].wait()
    x = hid_b[...].astype(F32)
    ms = jnp.mean(x * x, axis=-1, keepdims=True)
    normed = (x * lax.rsqrt(ms + EPSILON) * ngain_b[...]).astype(BF)
    normed_o[...] = normed
    copies[4].wait()
    k = jnp.dot(normed, wk_b[...], preferred_element_type=F32)
    copies[5].wait()
    v = jnp.dot(normed, wv_b[...], preferred_element_type=F32)
    for h in range(2):
        kv_o[0, :, h * HD:(h + 1) * HD] = head_norm_rope(
            k[:, h * HD:(h + 1) * HD], kgain_b[...], cos, sin)
    kv_o[1] = v.T.astype(BF)


def q_kernel(normed, wq, qgain, cos, sin, q_o, wq_b, acc, qgain_b, sems):
    depth = wq.shape[0]
    rows = depth // QBLOCKS
    copies = fetch([(qgain, qgain_b)] + [
        (wq.at[b * rows:(b + 1) * rows], wq_b.at[b * rows:(b + 1) * rows])
        for b in range(QBLOCKS)], sems)
    half = depth // 2
    width = 2 * HD
    blocks = wq.shape[1] // width
    for c in copies[:1 + QBLOCKS // 2]:
        c.wait()
    gain = jnp.broadcast_to(qgain_b[...], (TOK, HD)).T
    for b in range(blocks):
        cols = slice(b * width, (b + 1) * width)
        acc[:, cols] = jnp.dot(normed[:, :half], wq_b[:half, cols], preferred_element_type=F32)
    for c in copies[1 + QBLOCKS // 2:]:
        c.wait()
    for b in range(blocks):
        cols = slice(b * width, (b + 1) * width)
        q = acc[:, cols] + jnp.dot(normed[:, half:], wq_b[half:, cols], preferred_element_type=F32)
        for h in range(2):
            q_o[2 * b + h] = head_norm_rope_t(
                q[:, h * HD:(h + 1) * HD].T, gain, cos[...], sin[...])


def attend_kernel(table, first_stage, last_stage, *refs):
    slots = len(table)
    refs = list(refs)
    docs, q = refs[:2]
    refs = refs[2:]
    pieces, refs = list(refs[:slots]), refs[slots:]
    me = lax.axis_index("tok")
    role = lax.axis_index("role")
    if first_stage:
        own, refs = refs[0], refs[1:]
    else:
        m_in, acc_in = refs[:2]
        refs = refs[2:]
    if last_stage:
        wout, refs = refs[0], refs[1:]
        send_o, att, win, hops, m_s, acc_s = refs
    else:
        m_s, acc_s, win, hops = refs
    sources = pieces + ([own] if first_stage else [])
    for n, piece in enumerate(sources):
        win[n] = piece[...]
    if not first_stage:
        m_s[...] = m_in[...]
        acc_s[...] = acc_in[...]
    z = me % RING
    for n, row in enumerate(table):
        hop = jnp.int32(row[0])
        for zz in range(1, RING):
            hop = jnp.where(z == zz, jnp.int32(row[zz]), hop)
        hops[n] = hop
    step = 2 * BLK

    def tile(i, slot, lo, size, mask, first):
        units = [(g, j) for g in range(2) for j in range(4)]

        def scores(g, j):
            k = win[slot, 0, lo:lo + size, g * HD:(g + 1) * HD]
            qt = jnp.concatenate(
                [q[g * 8 + 2 * j + e, :, i * BLK:(i + 1) * BLK] for e in range(2)], axis=1)
            s = jnp.dot(k, qt, preferred_element_type=F32)
            return s if mask is None else jnp.where(mask, s, -1e30)

        ahead = [scores(*units[n]) for n in range(AHEAD)]
        for n, (g, j) in enumerate(units):
            s = ahead.pop(0)
            if n + AHEAD < len(units):
                ahead.append(scores(*units[n + AHEAD]))
            cols = slice(j * step, (j + 1) * step)
            v = win[slot, 1, g * HD:(g + 1) * HD, lo:lo + size]
            v1 = jnp.concatenate([v, jnp.ones((EXTRA, size), BF)], axis=0)
            top = jnp.max(s, axis=0, keepdims=True)
            if first:
                m_new = top
            else:
                m_old = m_s[i, g, :, cols]
                m_new = jnp.maximum(m_old, top)
            p = jnp.exp2((s - m_new) * SCALE2).astype(BF)
            pv = jnp.dot(v1, p, preferred_element_type=F32)
            if first:
                acc_s[i, g, :, cols] = pv
            else:
                acc_s[i, g, :, cols] = acc_s[i, g, :, cols] * jnp.exp2((m_old - m_new) * SCALE2) + pv
            m_s[i, g, :, cols] = m_new

    for i in range(2):
        block = me * 2 + i
        depth = block - doc_start(docs, block)
        if first_stage:
            size = BLK * (i + 1)
            key = lax.broadcasted_iota(jnp.int32, (size, step), 0)
            token = lax.broadcasted_iota(jnp.int32, (size, step), 1) % BLK
            mask = key <= token + i * BLK
            if i == 1:
                mask = mask & (key >= jnp.where(depth == 0, BLK, 0))
            tile(i, slots, 0, size, mask, True)

        @pl.loop(0, slots)
        def _(slot):
            hop = hops[slot]

            @pl.when((hop > 0) & (2 * hop + i <= depth))
            def _():
                tile(i, slot, 0, 2 * BLK, None, False)

            @pl.when((hop > 0) & (2 * hop + i == depth + 1))
            def _():
                tile(i, slot, BLK, BLK, None, False)

        if last_stage:
            for g in range(2):
                for h in range(8):
                    cols = slice(h * BLK, (h + 1) * BLK)
                    o = acc_s[i, g, :HD, cols] * (1.0 / acc_s[i, g, HD:HD + 1, cols])
                    att[i * BLK:(i + 1) * BLK, (g * 8 + h) * HD:(g * 8 + h + 1) * HD] = o.T.astype(BF)
    if last_stage:
        half = wout.shape[1] // 2
        theirs = pl.multiple_of((1 - role) * half, half)
        send_o[...] = jnp.dot(
            att[...], wout[:, pl.ds(theirs, half)], preferred_element_type=F32).astype(BF)


def keep_kernel(att, wout, keep_o):
    half = wout.shape[1] // 2
    mine = pl.multiple_of(lax.axis_index("role") * half, half)
    keep_o[...] = jnp.dot(att[...], wout[:, pl.ds(mine, half)], preferred_element_type=F32)


HBM = pl.BlockSpec(memory_space=pltpu.MemorySpace.HBM)
SMEM = pl.BlockSpec(memory_space=pltpu.MemorySpace.SMEM)
VM = pl.BlockSpec(memory_space=pltpu.MemorySpace.VMEM)


def shifted(value, by):
    peers = lax.axis_size("tok")
    return lax.ppermute(value, "tok", [(t, (t + by) % peers) for t in range(peers)])


def moved(value, rows, turn, senders=(0, 1, 2, 3)):
    peers = lax.axis_size("tok")
    pairs = []
    for t in range(peers):
        z = t % RING
        if z in senders:
            pairs.append((t, (t - z + (z + turn) % RING + rows * RING) % peers))
    return lax.ppermute(value, "tok", pairs)


NEAR = ((4, 4, 4, 4), (0, 1, 1, 1), (0, 0, 0, 3), (8, 8, 8, 8))
MID = ((1, 5, 5, 5), (3, 3, 3, 7), (2, 2, 6, 6))
FAR = ((6, 6, 2, 2), (7, 7, 7, 0), (5, 0, 0, 0))


def layer(hidden, doc_blocks, norm_gain, w_query, w_key, w_value, q_gain, k_gain, w_out):
    d = hidden.shape[1]
    hq = w_query.shape[1] // HD
    freq = THETA ** (-(np.arange(HD // 2, dtype=np.float32) * np.float32(2.0)) / np.float32(HD))
    freq = jnp.asarray(np.concatenate([freq, freq])[None].astype(np.float32))
    doc_blocks, hidden, norm_row, w_key, w_value, k_row, freq, q_row, w_query = (
        pltpu.with_memory_space_constraint(x, pltpu.MemorySpace.HBM)
        for x in (doc_blocks, hidden, norm_gain[None], w_key, w_value, k_gain[None], freq, q_gain[None], w_query))
    normed, kv, cos, sin = pl.pallas_call(
        kv_kernel,
        out_shape=(
            jax.ShapeDtypeStruct((TOK, d), BF),
            jax.ShapeDtypeStruct((2, TOK, 2 * HD), BF),
            jax.ShapeDtypeStruct((HD, TOK), F32),
            jax.ShapeDtypeStruct((HD, TOK), F32),
        ),
        in_specs=[SMEM] + [HBM] * 6,
        out_specs=[VM] * 4,
        scratch_shapes=[
            pltpu.VMEM((TOK, d), BF),
            pltpu.VMEM((1, d), F32),
            pltpu.VMEM(w_key.shape, BF),
            pltpu.VMEM(w_value.shape, BF),
            pltpu.VMEM((1, HD), F32),
            pltpu.VMEM((1, HD), F32),
            pltpu.SemaphoreType.DMA((6,)),
        ],
        cost_estimate=pl.CostEstimate(flops=540_000_000, transcendentals=0, bytes_accessed=4_000_000),
        name="kv_kernel",
        compiler_params=pltpu.CompilerParams(vmem_limit_bytes=16 << 20),
    )(doc_blocks, hidden, norm_row, w_key, w_value, k_row, freq)

    row1 = shifted(kv, RING)
    up1 = moved(kv, 0, 1)
    down1 = moved(kv, 0, -1)
    row2 = shifted(kv, 2 * RING)

    queries = pl.pallas_call(
        q_kernel,
        out_shape=jax.ShapeDtypeStruct((hq, HD, TOK), BF),
        in_specs=[VM, HBM, HBM, VM, VM],
        out_specs=VM,
        scratch_shapes=[
            pltpu.VMEM(w_query.shape, BF),
            pltpu.VMEM((TOK, w_query.shape[1]), F32),
            pltpu.VMEM((1, HD), F32),
            pltpu.SemaphoreType.DMA((QBLOCKS + 1,)),
        ],
        cost_estimate=pl.CostEstimate(flops=2_147_000_000, transcendentals=0, bytes_accessed=10_000_000),
        name="q_kernel",
        compiler_params=pltpu.CompilerParams(vmem_limit_bytes=24 << 20),
    )(normed, w_query, q_row, cos, sin)

    lower = lax.axis_index("tok") % RING < RING // 2
    mid = [shifted(up1, RING)]
    mid.append(shifted(down1, RING))
    mid.append(moved(row1, 0, 2))
    mixed = jnp.where(lower, kv, row2)
    far = [moved(mixed, 0, 2)]
    far.append(moved(row2, 0, -1, (1, 2, 3)))
    far.append(moved(row2, 0, 1, (3,)))
    state = (
        jax.ShapeDtypeStruct((2, 2, 1, 8 * BLK), F32),
        jax.ShapeDtypeStruct((2, 2, HD + EXTRA, 8 * BLK), F32),
    )

    def stage(table, operands, extra):
        return pl.pallas_call(
            functools.partial(attend_kernel, table, extra, False),
            out_shape=state,
            in_specs=[SMEM] + [VM] * (len(operands) + 1),
            out_specs=[VM, VM],
            scratch_shapes=[
                pltpu.VMEM((len(table) + extra, 2, TOK, 2 * HD), BF),
                pltpu.SMEM((len(table),), jnp.int32),
            ],
            cost_estimate=pl.CostEstimate(flops=6_000_000_000, transcendentals=0, bytes_accessed=6_000_000),
            compiler_params=pltpu.CompilerParams(vmem_limit_bytes=24 << 20),
        )(doc_blocks, queries, *operands)

    partial = stage(NEAR, [row1, up1, down1, row2, kv], True)
    partial = stage(MID, [*mid, *partial], False)
    half = w_out.shape[1] // 2
    send, att = pl.pallas_call(
        functools.partial(attend_kernel, FAR, False, True),
        out_shape=(
            jax.ShapeDtypeStruct((TOK, half), BF),
            jax.ShapeDtypeStruct((TOK, hq * HD), BF),
        ),
        in_specs=[SMEM] + [VM] * (len(FAR) + 4),
        out_specs=[VM, VM],
        scratch_shapes=[
            pltpu.VMEM((len(FAR), 2, TOK, 2 * HD), BF),
            pltpu.SMEM((len(FAR),), jnp.int32),
            pltpu.VMEM(state[0].shape, F32),
            pltpu.VMEM(state[1].shape, F32),
        ],
        cost_estimate=pl.CostEstimate(flops=9_000_000_000, transcendentals=0, bytes_accessed=14_000_000),
        name="attend_far",
        compiler_params=pltpu.CompilerParams(vmem_limit_bytes=28 << 20),
    )(doc_blocks, queries, *far, *partial, w_out)
    other = lax.ppermute(send, "role", [(0, 1), (1, 0)])
    keep = pl.pallas_call(
        keep_kernel,
        out_shape=jax.ShapeDtypeStruct((TOK, half), F32),
        in_specs=[VM, VM],
        out_specs=VM,
        cost_estimate=pl.CostEstimate(flops=2_000_000_000, transcendentals=0, bytes_accessed=6_000_000),
        name="keep_kernel",
        compiler_params=pltpu.CompilerParams(vmem_limit_bytes=12 << 20),
    )(att, w_out)
    return (keep + other.astype(F32)).astype(BF)


def solution(mesh):
    return jax.shard_map(
        layer,
        mesh=mesh,
        in_specs=(
            P("tok", None), P(), P(), P(None, "role"), P(None, "role"), P(None, "role"),
            P(), P(), P("role", None),
        ),
        out_specs=P("tok", "role"),
        check_vma=False,
    )
```
